8 devices in a mesh: dp: 2 (over z, y), stage: 4 (over x, core).
Axes of the slice: x: 2, y: 2, z: 1, core: 2. Of those that a mesh axis runs over, the one named last changes fastest.
Arguments:
- tokens_in: bfloat16 [32, 1024, 768], P('dp'), parts along dimension 0
- targets: bfloat16 [32, 1024, 768], P('dp'), parts along dimension 0
- w_in: bfloat16 [8, 768, 3072], P('stage')
- w_out: bfloat16 [8, 3072, 768], P('stage')
- norm_gains: float32 [8, 768], P('stage')
Outputs:
- output 1: float32 [16, 768, 3072], P(('dp', 'stage')), parts along dimension 0
- output 2: float32 [16, 3072, 768], P(('dp', 'stage')), parts along dimension 0
- output 3: float32 [16, 768], P(('dp', 'stage')), parts along dimension 0
- output 4: float32 [2], P('dp'), parts along dimension 0
There are 2 independent parts. The reference program is written for one: setup_inputs(seed, part) draws one part's arguments, and reference() takes and returns one part's arrays. A program takes and returns all parts, laid end to end along the dimension named above; an argument that names none is the same for every part.
All inputs are finite; a program needn't handle non-finite values.
Results may differ from the reference program's by a relative error of at most 0.00215886.
Values are sent between devices in bfloat16 or wider.
A program may use at most 1 GiB of HBM per device.

```python
import jax
import jax.numpy as jnp
from jax import lax

STAGES = 4
SEGMENT_LAYERS = 1
MICRO_BATCHES = 16
MICRO_TOKENS = 1024
D_MODEL = 768
D_FF = 3072
LAYERS = 2 * STAGES * SEGMENT_LAYERS
EPSILON = 1e-6


def setup_inputs(seed: int = 0, part: int = 0) -> dict:
    base_key = jax.random.key(seed)
    key_list = jax.random.split(base_key, 4)
    data_key = jax.random.fold_in(key_list[0], part)
    key_tokens, key_targets = jax.random.split(data_key)
    shape_act = (MICRO_BATCHES, MICRO_TOKENS, D_MODEL)
    target_scale = (1.0 + 0.5 * LAYERS) ** 0.5
    tokens_in = jax.random.normal(key_tokens, shape_act, jnp.float32)
    targets = target_scale * jax.random.normal(key_targets, shape_act, jnp.float32)
    w_in = jax.random.normal(key_list[1], (LAYERS, D_MODEL, D_FF), jnp.float32) * D_MODEL ** -0.5
    w_out = jax.random.normal(key_list[2], (LAYERS, D_FF, D_MODEL), jnp.float32) * D_FF ** -0.5
    norm_gains = 1.0 + 0.5 * jax.random.normal(key_list[3], (LAYERS, D_MODEL), jnp.float32)
    return {
        'tokens_in': tokens_in.astype(jnp.bfloat16),
        'targets': targets.astype(jnp.bfloat16),
        'w_in': w_in.astype(jnp.bfloat16),
        'w_out': w_out.astype(jnp.bfloat16),
        'norm_gains': norm_gains,
    }


def norm_scale(x_f32, gain_vec):
    inv_rms = lax.rsqrt(jnp.mean(x_f32 * x_f32, axis=-1, keepdims=True) + EPSILON)
    return x_f32 * inv_rms * gain_vec


def layer_forward(x_act, first_w, second_w, gain_vec):
    x_f32 = x_act.astype(jnp.float32)
    normed = norm_scale(x_f32, gain_vec).astype(jnp.bfloat16)
    pre_act = jnp.dot(normed, first_w, preferred_element_type=jnp.float32)
    hidden = jax.nn.gelu(pre_act).astype(jnp.bfloat16)
    out_f32 = jnp.dot(hidden, second_w, preferred_element_type=jnp.float32)
    return (x_f32 + out_f32).astype(jnp.bfloat16)


def layer_backward(x_act, grad_h, first_w, second_w, gain_vec):
    x_f32 = x_act.astype(jnp.float32)
    normed_f32, norm_vjp = jax.vjp(norm_scale, x_f32, gain_vec)
    normed = normed_f32.astype(jnp.bfloat16)
    pre_act = jnp.dot(normed, first_w, preferred_element_type=jnp.float32)
    hidden_f32, gelu_vjp = jax.vjp(jax.nn.gelu, pre_act)
    hidden = hidden_f32.astype(jnp.bfloat16)
    grad_second = jnp.dot(hidden.T, grad_h, preferred_element_type=jnp.float32)
    grad_hidden = jnp.dot(grad_h, second_w.T, preferred_element_type=jnp.float32)
    grad_pre = gelu_vjp(grad_hidden)[0].astype(jnp.bfloat16)
    grad_first = jnp.dot(normed.T, grad_pre, preferred_element_type=jnp.float32)
    grad_normed = jnp.dot(grad_pre, first_w.T, preferred_element_type=jnp.float32)
    grad_x_norm, grad_gain = norm_vjp(grad_normed)
    grad_x = (grad_h.astype(jnp.float32) + grad_x_norm).astype(jnp.bfloat16)
    return grad_x, grad_first, grad_second, grad_gain


def to_exec_order(stored):
    tail_shape = stored.shape[1:]
    blocks = stored.reshape((STAGES, 2, SEGMENT_LAYERS) + tail_shape)
    down_half = blocks[:, 0].reshape((STAGES * SEGMENT_LAYERS,) + tail_shape)
    up_half = blocks[::-1, 1].reshape((STAGES * SEGMENT_LAYERS,) + tail_shape)
    return jnp.concatenate([down_half, up_half], axis=0)


def to_stored_order(in_exec):
    tail_shape = in_exec.shape[1:]
    half_rows = STAGES * SEGMENT_LAYERS
    down_half = in_exec[:half_rows].reshape((STAGES, SEGMENT_LAYERS) + tail_shape)
    up_half = in_exec[half_rows:].reshape((STAGES, SEGMENT_LAYERS) + tail_shape)[::-1]
    return jnp.stack([down_half, up_half], axis=1).reshape((LAYERS,) + tail_shape)


def reference(tokens_in, targets, w_in, w_out, norm_gains):
    first_all = to_exec_order(w_in)
    second_all = to_exec_order(w_out)
    gain_all = to_exec_order(norm_gains)
    seed_scale = 2.0 / (MICRO_BATCHES * MICRO_TOKENS)

    def micro_step(loop_state, micro_pair):
        sum_first, sum_second, sum_gain, sse_total = loop_state
        micro_tokens, micro_targets = micro_pair

        def forward_layer(act_in, layer_weights):
            return layer_forward(act_in, layer_weights[0], layer_weights[1], layer_weights[2]), act_in

        final_act, saved_inputs = lax.scan(forward_layer, micro_tokens, (first_all, second_all, gain_all))
        error_f32 = final_act.astype(jnp.float32) - micro_targets.astype(jnp.float32)
        seed_grad = (error_f32 * seed_scale).astype(jnp.bfloat16)

        def backward_layer(grad_h, layer_data):
            grad_x, grad_first, grad_second, grad_gain = layer_backward(
                layer_data[0], grad_h, layer_data[1], layer_data[2], layer_data[3])
            return grad_x, (grad_first, grad_second, grad_gain)

        _, layer_grads = lax.scan(backward_layer, seed_grad,
                                  (saved_inputs, first_all, second_all, gain_all), reverse=True)
        new_state = (sum_first + layer_grads[0], sum_second + layer_grads[1],
                     sum_gain + layer_grads[2], sse_total + jnp.sum(error_f32 * error_f32))
        return new_state, None

    init_state = (jnp.zeros((LAYERS, D_MODEL, D_FF), jnp.float32),
                  jnp.zeros((LAYERS, D_FF, D_MODEL), jnp.float32),
                  jnp.zeros((LAYERS, D_MODEL), jnp.float32),
                  jnp.zeros((), jnp.float32))
    final_state, _ = lax.scan(micro_step, init_state, (tokens_in, targets))
    loss_value = final_state[3] / (MICRO_BATCHES * MICRO_TOKENS * D_MODEL)
    return (to_stored_order(final_state[0]), to_stored_order(final_state[1]),
            to_stored_order(final_state[2]), loss_value.reshape(1))
```

```python
import functools

import jax
import jax.numpy as jnp
from jax import lax
from jax.experimental import pallas as pl
from jax.experimental.pallas import tpu as pltpu
from jax.sharding import PartitionSpec as P

EPSILON = 1e-6
GELU_A = 0.7978845608028654
GELU_B = 0.7978845608028654 * 0.044715
CHUNK = 512
F_FWD = 512
F_BWD = 256
N_BLK = 256
VMEM_LIMIT = 67_043_328
BF16 = jnp.bfloat16
F32 = jnp.float32


def dot(a, b):
    return jnp.dot(a, b, preferred_element_type=F32)


def dot_rt(a, b):
    return lax.dot_general(a, b, (((1,), (1,)), ((), ())), preferred_element_type=F32)


def inverse_rms(x_f32):
    return lax.rsqrt(jnp.mean(x_f32 * x_f32, axis=-1, keepdims=True) + EPSILON)


def gelu_of(a):
    t = jnp.tanh(a * (GELU_A + GELU_B * (a * a)))
    h = 0.5 * a
    return h + h * t


def gelu_and_slope(a):
    a2 = a * a
    t = jnp.tanh(a * (GELU_A + GELU_B * a2))
    h = 0.5 * a
    slope = (0.5 + 0.5 * t) + h * (1.0 - t * t) * (GELU_A + (3.0 * GELU_B) * a2)
    return h + h * t, slope


def fold_rows(v):
    return jnp.sum(v.reshape(v.shape[0] // 8, 8, v.shape[1]), axis=0)


def enter(stage, stages):
    barrier = pltpu.get_barrier_semaphore()
    for step in (1, stages - 1):
        pl.semaphore_signal(barrier, inc=1, device_id={"stage": lax.rem(stage + step, stages)},
                            device_id_type=pl.DeviceIdType.MESH)
    pl.semaphore_wait(barrier, 2)


def run_schedule(stage, stages, count, lag, most_lag, land, outs, send, recv, issue, first_half, second_half,
                 finish, wait_finish, midway):
    last = stages - 1

    def place(k):
        p = lax.rem(k, 2)
        c = lax.div(k, 2) - p * lag
        return p, c, (c >= 0) & (c < count)

    def hop(p, c):
        return pltpu.make_async_remote_copy(
            src_ref=outs.at[p], dst_ref=land.at[p, c], send_sem=send.at[p], recv_sem=recv.at[p, c],
            device_id={"stage": stage + 1 - 2 * p}, device_id_type=pl.DeviceIdType.MESH)

    def turn(c):
        return pltpu.make_async_copy(outs.at[0], land.at[1, c], recv.at[1, c])

    def leaves(p):
        return ((p == 0) & (stage < last)) | ((p == 1) & (stage > 0))

    def arrived(p, c):
        pltpu.make_async_copy(outs.at[p], land.at[p, c], recv.at[p, c]).wait()

    def step(k, carry):
        p, c, valid = place(k)
        p_next, c_next, valid_next = place(k + 1)

        @pl.when(valid)
        def _():
            first_half(p, c)

        @pl.when(valid_next)
        def _():
            @pl.when((p_next == 1) | (stage > 0))
            def _():
                arrived(p_next, c_next)
            issue(p_next, c_next)

        midway(k)

        @pl.when(valid)
        def _():
            @pl.when((c >= 1) & leaves(p))
            def _():
                hop(p, c).wait_send()

            @pl.when((c >= 1) & (p == 1) & (stage == 0))
            def _():
                wait_finish(c)
            second_half(p, c)

            @pl.when(leaves(p))
            def _():
                hop(p, c).start()

            @pl.when((p == 0) & (stage == last))
            def _():
                turn(c).start()

            @pl.when((p == 1) & (stage == 0))
            def _():
                finish(c)
        return carry

    @pl.when(stage > 0)
    def _():
        arrived(0, 0)
    issue(0, 0)
    lax.fori_loop(0, 2 * (count + most_lag), step, 0)

    @pl.when(stage < last)
    def _():
        hop(0, count - 1).wait_send()

    @pl.when(stage > 0)
    def _():
        hop(1, count - 1).wait_send()

    @pl.when(stage == 0)
    def _():
        wait_finish(count - 1)


def forward_kernel(stages, seed_scale, tokens, targets, w_in, w_out, gains, land, seeds, sse,
                   wi, wo, xs, outs, tgt, normed, hidden, w_sem, ld_sem, tgt_sem, fin_sem, send, recv):
    stage = lax.axis_index("stage")
    count, _, d_model = tokens.shape
    d_ff = wi.shape[2]
    lag = (stages - 1 - stage) * 3 + 1
    most_lag = (stages - 1) * 3 + 1
    loads = [pltpu.make_async_copy(w_in, wi, w_sem.at[0]), pltpu.make_async_copy(w_out, wo, w_sem.at[1])]
    for load in loads:
        load.start()
    sse[...] = jnp.zeros_like(sse)
    enter(stage, stages)

    def tgt_load(c):
        return pltpu.make_async_copy(targets.at[c], tgt, tgt_sem)

    def issue(p, c):
        @pl.when((p == 0) & (stage == 0))
        def _():
            pltpu.make_async_copy(tokens.at[c], xs.at[p], ld_sem.at[p]).start()

        @pl.when((p == 1) | (stage > 0))
        def _():
            pltpu.make_async_copy(land.at[p, c], xs.at[p], ld_sem.at[p]).start()

        @pl.when((p == 1) & (stage == 0))
        def _():
            tgt_load(c).start()

    for load in loads:
        load.wait()

    def first_half(p, c):
        pltpu.make_async_copy(land.at[p, c], xs.at[p], ld_sem.at[p]).wait()
        x = xs[p].astype(F32)
        normed[...] = (x * inverse_rms(x) * gains[p]).astype(BF16)
        for f in range(0, d_ff, F_FWD):
            a = dot(normed[...], wi[p, :, f:f + F_FWD])
            hidden[:, f:f + F_FWD] = gelu_of(a).astype(BF16)

    def second_half(p, c):
        for n in range(0, d_model, N_BLK):
            cols = slice(n, n + N_BLK)
            out = dot(hidden[...], wo[p, :, cols])
            outs[p, :, cols] = (xs[p, :, cols].astype(F32) + out).astype(BF16)

        @pl.when((p == 1) & (stage == 0))
        def _():
            tgt_load(c).wait()
            error = outs[1].astype(F32) - tgt[...].astype(F32)
            sse[...] += fold_rows(error * error)
            outs[1] = (error * seed_scale).astype(BF16)

    def seed_store(c):
        return pltpu.make_async_copy(outs.at[1], seeds.at[c], fin_sem)

    run_schedule(stage, stages, count, lag, most_lag, land, outs, send, recv, issue, first_half, second_half,
                 lambda c: seed_store(c).start(), lambda c: seed_store(c).wait(), lambda k: None)


def backward_kernel(stages, tokens, saved, seeds, w_in, w_out, gains, land, grad_in, grad_out_t, grad_gain,
                    wi, wo_first, wo_ring, acc_in, acc_out, xs, dhs, outs, normed, normed_t, dh_t, dn, hidden, da,
                    w_sem, ring_sem, x_sem, dh_sem, flush_sem, send, recv):
    stage = lax.axis_index("stage")
    count, _, d_model = tokens.shape
    d_ff = wi.shape[2]
    blocks = d_ff // F_BWD
    lag = ((stages - 1 - stage) * 5) // 2 + 1
    most_lag = ((stages - 1) * 5) // 2 + 1
    loads = [pltpu.make_async_copy(w_in, wi, w_sem.at[0]),
             pltpu.make_async_copy(w_out.at[0, pl.ds(0, F_BWD)], wo_first.at[0], w_sem.at[1]),
             pltpu.make_async_copy(w_out.at[1, pl.ds(0, F_BWD)], wo_first.at[1], w_sem.at[2])]
    for load in loads:
        load.start()
    grad_gain[...] = jnp.zeros_like(grad_gain)

    def clear(i, carry):
        rows = pl.ds(pl.multiple_of(i * 8, 8), 8)
        for row in range(2):
            acc_in[row, rows, :] = jnp.zeros((8, d_ff), F32)
            acc_out[row, rows, :] = jnp.zeros((8, d_ff), F32)
        return carry

    lax.fori_loop(0, d_model // 8, clear, 0)
    enter(stage, stages)

    def issue(p, c):
        @pl.when((p == 0) & (stage == 0))
        def _():
            pltpu.make_async_copy(seeds.at[c], dhs.at[p], dh_sem.at[p]).start()

        @pl.when((p == 1) | (stage > 0))
        def _():
            pltpu.make_async_copy(land.at[p, c], dhs.at[p], dh_sem.at[p]).start()

        @pl.when((p == 1) & (stage == 0))
        def _():
            pltpu.make_async_copy(tokens.at[c], xs.at[p], x_sem.at[p]).start()

        @pl.when((p == 0) | (stage > 0))
        def _():
            pltpu.make_async_copy(saved.at[1 - p, c], xs.at[p], x_sem.at[p]).start()

    for load in loads:
        load.wait()

    def ring_load(row, block):
        return pltpu.make_async_copy(w_out.at[row, pl.ds(block * F_BWD, F_BWD)], wo_ring.at[block % 3],
                                     ring_sem.at[block % 3])

    def weight_grads(row, block):
        cols = slice(block * F_BWD, (block + 1) * F_BWD)
        acc_out[row, :, cols] += dot(dh_t[...], hidden[block % 2])
        acc_in[row, :, cols] += dot(normed_t[...], da[:, cols])

    def first_half(p, c):
        row = 1 - p
        ring_load(row, 1).start()
        ring_load(row, 2).start()
        pltpu.make_async_copy(land.at[p, c], dhs.at[p], dh_sem.at[p]).wait()
        pltpu.make_async_copy(saved.at[1 - p, c], xs.at[p], x_sem.at[p]).wait()
        x = xs[p].astype(F32)
        n = (x * inverse_rms(x) * gains[row]).astype(BF16)
        normed[...] = n
        normed_t[...] = n.T
        dh_t[...] = dhs[p].T
        for block in range(blocks):
            cols = slice(block * F_BWD, (block + 1) * F_BWD)
            if block:
                ring_load(row, block).wait()
                if block + 2 < blocks:
                    ring_load(row, block + 2).start()
            wo_block = wo_ring[block % 3] if block else wo_first[row]
            du = dot_rt(dhs[p], wo_block)
            a = dot(normed[...], wi[row, :, cols])
            if block:
                weight_grads(row, block - 1)
            u, slope = gelu_and_slope(a)
            hidden[block % 2] = u.astype(BF16)
            da[:, cols] = (du * slope).astype(BF16)

    def second_half(p, c):
        row = 1 - p
        for n in range(0, d_model, N_BLK):
            dn[:, n:n + N_BLK] = dot_rt(da[...], wi[row, n:n + N_BLK, :])
        weight_grads(row, blocks - 1)
        x = xs[p].astype(F32)
        inv = inverse_rms(x)
        grad_n = dn[...]
        xr = x * inv
        grad_gain[row] += fold_rows(xr * grad_n)
        scaled = grad_n * gains[row]
        mean = jnp.mean(xr * scaled, axis=-1, keepdims=True)
        outs[p] = (dhs[p].astype(F32) + inv * (scaled - xr * mean)).astype(BF16)

    def flushes(row):
        return [pltpu.make_async_copy(acc_in.at[row], grad_in.at[row], flush_sem.at[0, row]),
                pltpu.make_async_copy(acc_out.at[row], grad_out_t.at[row], flush_sem.at[1, row])]

    def midway(k):
        @pl.when(k == 2 * count)
        def _():
            for flush in flushes(1):
                flush.start()

    run_schedule(stage, stages, count, lag, most_lag, land, outs, send, recv, issue, first_half, second_half,
                 lambda c: None, lambda c: None, midway)
    for flush in flushes(0):
        flush.start()
    for row in (1, 0):
        for flush in flushes(row):
            flush.wait()


def solution(mesh):
    stages = mesh.shape['stage']

    def device_step(tokens, targets, w_in, w_out, norm_gains):
        micro_count, tokens_mb, d_model = tokens.shape
        d_ff = w_in.shape[2]
        total = micro_count * tokens_mb
        count = total // CHUNK
        tokens = tokens.reshape(count, CHUNK, d_model)
        targets = targets.reshape(count, CHUNK, d_model)
        gains = norm_gains.reshape(2, 1, d_model)
        any_spec = pl.BlockSpec(memory_space=pl.ANY)
        vmem_spec = pl.BlockSpec(memory_space=pltpu.VMEM)
        dma = pltpu.SemaphoreType.DMA
        flops = 2 * 2 * total * d_model * d_ff
        land_shape = jax.ShapeDtypeStruct((2, count, CHUNK, d_model), BF16)

        saved, seeds, sse = pl.pallas_call(
            functools.partial(forward_kernel, stages, 2.0 / total),
            out_shape=(land_shape, jax.ShapeDtypeStruct((count, CHUNK, d_model), BF16),
                       jax.ShapeDtypeStruct((8, d_model), F32)),
            in_specs=[any_spec] * 4 + [vmem_spec],
            out_specs=(any_spec, any_spec, vmem_spec),
            scratch_shapes=[
                pltpu.VMEM((2, d_model, d_ff), BF16), pltpu.VMEM((2, d_ff, d_model), BF16),
                pltpu.VMEM((2, CHUNK, d_model), BF16), pltpu.VMEM((2, CHUNK, d_model), BF16),
                pltpu.VMEM((CHUNK, d_model), BF16), pltpu.VMEM((CHUNK, d_model), BF16),
                pltpu.VMEM((CHUNK, d_ff), BF16),
                dma((2,)), dma((2,)), dma, dma, dma((2,)), dma((2, count)),
            ],
            compiler_params=pltpu.CompilerParams(collective_id=0, has_side_effects=True,
                                                 vmem_limit_bytes=VMEM_LIMIT),
            cost_estimate=pl.CostEstimate(flops=2 * flops, bytes_accessed=10 ** 8, transcendentals=0),
        )(tokens, targets, w_in, w_out, gains)

        _, grad_in, grad_out_t, grad_gain = pl.pallas_call(
            functools.partial(backward_kernel, stages),
            out_shape=(land_shape, jax.ShapeDtypeStruct((2, d_model, d_ff), F32),
                       jax.ShapeDtypeStruct((2, d_model, d_ff), F32),
                       jax.ShapeDtypeStruct((2, 8, d_model), F32)),
            in_specs=[any_spec] * 5 + [vmem_spec],
            out_specs=(any_spec, any_spec, any_spec, vmem_spec),
            scratch_shapes=[
                pltpu.VMEM((2, d_model, d_ff), BF16),
                pltpu.VMEM((2, F_BWD, d_model), BF16), pltpu.VMEM((3, F_BWD, d_model), BF16),
                pltpu.VMEM((2, d_model, d_ff), F32), pltpu.VMEM((2, d_model, d_ff), F32),
                pltpu.VMEM((2, CHUNK, d_model), BF16), pltpu.VMEM((2, CHUNK, d_model), BF16),
                pltpu.VMEM((2, CHUNK, d_model), BF16),
                pltpu.VMEM((CHUNK, d_model), BF16),
                pltpu.VMEM((d_model, CHUNK), BF16), pltpu.VMEM((d_model, CHUNK), BF16),
                pltpu.VMEM((CHUNK, d_model), F32),
                pltpu.VMEM((2, CHUNK, F_BWD), BF16), pltpu.VMEM((CHUNK, d_ff), BF16),
                dma((3,)), dma((3,)), dma((2,)), dma((2,)), dma((2, 2)), dma((2,)), dma((2, count)),
            ],
            compiler_params=pltpu.CompilerParams(collective_id=1, has_side_effects=True,
                                                 vmem_limit_bytes=VMEM_LIMIT),
            cost_estimate=pl.CostEstimate(flops=5 * flops, bytes_accessed=10 ** 8, transcendentals=0),
        )(tokens, saved, seeds, w_in, w_out, gains)

        loss_value = lax.psum(jnp.sum(sse), 'stage') / (total * d_model)
        return grad_in, jnp.swapaxes(grad_out_t, 1, 2), jnp.sum(grad_gain, axis=1), loss_value.reshape(1)

    block_spec = P(('dp', 'stage'))
    return jax.shard_map(device_step, mesh=mesh,
                         in_specs=(P('dp'), P('dp'), P('stage'), P('stage'), P('stage')),
                         out_specs=(block_spec, block_spec, block_spec, P('dp')),
                         check_vma=False)
```

```python
import functools

import jax
import jax.numpy as jnp
from jax import lax
from jax.experimental import pallas as pl
from jax.experimental.pallas import tpu as pltpu
from jax.sharding import PartitionSpec as P

EPSILON = 1e-6
GELU_A = 0.7978845608028654
GELU_B = 0.7978845608028654 * 0.044715
CHUNK = 512
F_BLK = 256
FWD_SPLIT = 8
N_BLK = 256
VMEM_LIMIT = 67_043_328
LAGS = (3, 1, 2)
BF16 = jnp.bfloat16
F32 = jnp.float32


def dot(a, b):
    return jnp.dot(a, b, preferred_element_type=F32)


def dot_rt(a, b):
    return lax.dot_general(a, b, (((1,), (1,)), ((), ())), preferred_element_type=F32)


def inverse_rms(x_f32):
    return lax.rsqrt(jnp.mean(x_f32 * x_f32, axis=-1, keepdims=True) + EPSILON)


def gelu_of(a):
    t = jnp.tanh(a * (GELU_A + GELU_B * (a * a)))
    h = 0.5 * a
    return h + h * t


def gelu_and_slope(a):
    a2 = a * a
    t = jnp.tanh(a * (GELU_A + GELU_B * a2))
    h = 0.5 * a
    slope = (0.5 + 0.5 * t) + h * (1.0 - t * t) * (GELU_A + (3.0 * GELU_B) * a2)
    return h + h * t, slope


def fold_rows(v):
    return jnp.sum(v.reshape(v.shape[0] // 8, 8, v.shape[1]), axis=0)


def enter(stage, stages):
    barrier = pltpu.get_barrier_semaphore()
    for step in (1, stages - 1):
        pl.semaphore_signal(barrier, inc=1, device_id={"stage": lax.rem(stage + step, stages)},
                            device_id_type=pl.DeviceIdType.MESH)
    pl.semaphore_wait(barrier, 2)


def train_kernel(stages, seed_scale, lags, tokens, targets, w_in, w_out, gains, land, grad_in, grad_out_t,
                 grad_gain, sse, wi, wo_first, wo_ring, acc_in, acc_out, xs, dhs, outs, normed, normed_t, dh_t, sums,
                 hidden, da, w_sem, ring_sem, x_sem, dh_sem, flush_sem, send, recv):
    stage = lax.axis_index("stage")
    last = stages - 1
    count, _, d_model = tokens.shape
    d_ff = wi.shape[2]
    blocks = d_ff // F_BLK
    up_gap, back_gap, home_gap = lags
    lag_1 = (last - stage) * up_gap + 1
    lag_2 = last * up_gap + 2 + stage * back_gap
    lag_3 = last * (up_gap + back_gap) + 3 + (last - stage) * home_gap
    most_lag = last * (up_gap + back_gap + home_gap) + 3
    loads = [pltpu.make_async_copy(w_in, wi, w_sem.at[0]),
             pltpu.make_async_copy(w_out.at[0, pl.ds(0, F_BLK)], wo_first.at[0], w_sem.at[1]),
             pltpu.make_async_copy(w_out.at[1, pl.ds(0, F_BLK)], wo_first.at[1], w_sem.at[2])]
    for load in loads:
        load.start()
    grad_gain[...] = jnp.zeros_like(grad_gain)
    sse[...] = jnp.zeros_like(sse)
    enter(stage, stages)

    def place(k):
        q = lax.rem(k + 4, 4)
        tick = lax.div(k + 4, 4) - 1
        lag = jnp.where(q == 0, 0, jnp.where(q == 1, lag_1, jnp.where(q == 2, lag_2, lag_3)))
        c = tick - lag
        return q, c, (c >= 0) & (c < count)

    def row_of(q):
        return jnp.where((q == 0) | (q == 3), 0, 1)

    def hop(q, c):
        return pltpu.make_async_remote_copy(
            src_ref=outs.at[lax.rem(q, 2)], dst_ref=land.at[q, c], send_sem=send.at[q], recv_sem=recv.at[q, c],
            device_id={"stage": stage + 1 - 2 * lax.rem(q, 2)}, device_id_type=pl.DeviceIdType.MESH)

    def turn(q, c):
        return pltpu.make_async_copy(outs.at[lax.rem(q, 2)], land.at[q + 1, c], recv.at[q + 1, c])

    def leaves(q):
        p = lax.rem(q, 2)
        return ((p == 0) & (stage < last)) | ((p == 1) & (stage > 0))

    def turns(q):
        return ((lax.rem(q, 2) == 0) & (stage == last)) | ((q == 1) & (stage == 0))

    def from_turn(q):
        return ((lax.rem(q, 2) == 1) & (stage == last)) | ((q == 2) & (stage == 0))

    def arrived(q, c):
        pltpu.make_async_copy(outs.at[lax.rem(q, 2)], land.at[q, c], recv.at[q, c]).wait()

    def x_load(q, c):
        return pltpu.make_async_copy(land.at[row_of(q), c], xs.at[lax.rem(q, 2)], x_sem.at[lax.rem(q, 2)])

    def dh_load(q, c):
        return pltpu.make_async_copy(land.at[q, c], dhs.at[lax.rem(q, 2)], dh_sem.at[lax.rem(q, 2)])

    def issue(q, c):
        from_tokens = (row_of(q) == 0) & (stage == 0)

        @pl.when(from_tokens)
        def _():
            pltpu.make_async_copy(tokens.at[c], xs.at[lax.rem(q, 2)], x_sem.at[lax.rem(q, 2)]).start()

        @pl.when(jnp.logical_not(from_tokens))
        def _():
            x_load(q, c).start()

        @pl.when(q >= 2)
        def _():
            dh_load(q, c).start()

        @pl.when((q == 1) & (stage == 0))
        def _():
            pltpu.make_async_copy(targets.at[c], dhs.at[1], dh_sem.at[1]).start()

    def ring_load(row, block):
        return pltpu.make_async_copy(w_out.at[row, pl.ds(block * F_BLK, F_BLK)], wo_ring.at[block % 3],
                                     ring_sem.at[block % 3])

    def w_out_block(row, block):
        return wo_ring[block % 3] if block else wo_first[row]

    def columns(block):
        return slice(block * F_BLK, (block + 1) * F_BLK)

    def project(row, block):
        part = dot(hidden[block % 2], w_out_block(row, block))
        if block:
            sums[...] += part
        else:
            sums[...] = part

    def forward_block(row, block):
        if block >= 2:
            ring_load(row, block - 1).wait()
        if block + 1 < blocks:
            ring_load(row, block + 1).start()
        a = dot(normed[...], wi[row, :, columns(block)])
        if block:
            project(row, block - 1)
        hidden[block % 2] = gelu_of(a).astype(BF16)

    def forward_first(q, c):
        row = row_of(q)
        x_load(q, c).wait()
        x = xs[lax.rem(q, 2)].astype(F32)
        normed[...] = (x * inverse_rms(x) * gains[row]).astype(BF16)
        for block in range(FWD_SPLIT):
            forward_block(row, block)

    def forward_second(q, c):
        row = row_of(q)
        for block in range(FWD_SPLIT, blocks):
            forward_block(row, block)
        ring_load(row, blocks - 1).wait()
        out = sums[...] + dot(hidden[(blocks - 1) % 2], w_out_block(row, blocks - 1))
        outs[lax.rem(q, 2)] = (xs[lax.rem(q, 2)].astype(F32) + out).astype(BF16)

        @pl.when((q == 1) & (stage == 0))
        def _():
            dh_load(q, c).wait()
            error = outs[1].astype(F32) - dhs[1].astype(F32)
            sse[...] += fold_rows(error * error)
            outs[1] = (error * seed_scale).astype(BF16)

    def weight_grads(row, block):
        cols = columns(block)
        acc_out[row, :, cols] += dot(dh_t[...], hidden[block % 2])
        acc_in[row, :, cols] += dot(normed_t[...], da[:, cols])

    def clear():
        def piece(i, carry):
            rows = pl.ds(pl.multiple_of(i * 8, 8), 8)
            for row in range(2):
                acc_in[row, rows, :] = jnp.zeros((8, d_ff), F32)
                acc_out[row, rows, :] = jnp.zeros((8, d_ff), F32)
            return carry
        lax.fori_loop(0, d_model // 8, piece, 0)

    def backward_first(q, c):
        row = row_of(q)
        slot = lax.rem(q, 2)
        ring_load(row, 1).start()
        ring_load(row, 2).start()

        dh_load(q, c).wait()
        x_load(q, c).wait()
        x = xs[slot].astype(F32)
        n = (x * inverse_rms(x) * gains[row]).astype(BF16)
        normed[...] = n
        normed_t[...] = n.T
        dh_t[...] = dhs[slot].T
        for block in range(blocks):
            if block:
                ring_load(row, block).wait()
                if block + 2 < blocks:
                    ring_load(row, block + 2).start()
            du = dot_rt(dhs[slot], w_out_block(row, block))
            a = dot(normed[...], wi[row, :, columns(block)])
            if block:
                weight_grads(row, block - 1)
            u, slope = gelu_and_slope(a)
            hidden[block % 2] = u.astype(BF16)
            da[:, columns(block)] = (du * slope).astype(BF16)

    def backward_second(q, c):
        row = row_of(q)
        slot = lax.rem(q, 2)
        for n in range(0, d_model, N_BLK):
            sums[:, n:n + N_BLK] = dot_rt(da[...], wi[row, n:n + N_BLK, :])
        weight_grads(row, blocks - 1)
        x = xs[slot].astype(F32)
        inv = inverse_rms(x)
        grad_n = sums[...]
        xr = x * inv
        grad_gain[row] += fold_rows(xr * grad_n)
        scaled = grad_n * gains[row]
        mean = jnp.mean(xr * scaled, axis=-1, keepdims=True)
        outs[slot] = (dhs[slot].astype(F32) + inv * (scaled - xr * mean)).astype(BF16)

    def flushes(row):
        return [pltpu.make_async_copy(acc_in.at[row], grad_in.at[row], flush_sem.at[0, row]),
                pltpu.make_async_copy(acc_out.at[row], grad_out_t.at[row], flush_sem.at[1, row])]

    def step(k, carry):
        q, c, valid = place(k)
        q_next, c_next, valid_next = place(k + 1)

        @pl.when(valid & (q < 2))
        def _():
            forward_first(q, c)

        @pl.when(valid & (q >= 2))
        def _():
            backward_first(q, c)

        q_prev, c_prev, valid_prev = place(k - 1)

        @pl.when(valid_prev & turns(q_prev))
        def _():
            turn(q_prev, c_prev).wait()

        @pl.when(valid_next)
        def _():
            @pl.when(((q_next > 0) | (stage > 0)) & jnp.logical_not(from_turn(q_next)))
            def _():
                arrived(q_next, c_next)
            issue(q_next, c_next)

        @pl.when((k == 1) & (stage == 0))
        def _():
            clear()

        @pl.when(k == 4 * (count + lag_2))
        def _():
            for flush in flushes(1):
                flush.start()

        q_slot, c_slot, used_slot = place(k - 2)

        @pl.when(valid & used_slot & leaves(q))
        def _():
            hop(q_slot, c_slot).wait_send()

        @pl.when(valid & jnp.logical_not(used_slot) & (c >= 1) & leaves(q))
        def _():
            hop(q, c - 1).wait_send()

        @pl.when(valid & (q < 2))
        def _():
            forward_second(q, c)

        @pl.when(valid & (q >= 2))
        def _():
            backward_second(q, c)

        @pl.when(valid & leaves(q))
        def _():
            hop(q, c).start()

        @pl.when(valid & turns(q))
        def _():
            turn(q, c).start()
        return carry

    @pl.when(stage > 0)
    def _():
        clear()
    for load in loads:
        load.wait()

    @pl.when(stage > 0)
    def _():
        arrived(0, 0)
    issue(0, 0)
    lax.fori_loop(0, 4 * (count + most_lag), step, 0)
    for flush in flushes(0):
        flush.start()
    for q in (2, 3):
        @pl.when(leaves(q))
        def _(q=q):
            hop(q, count - 1).wait_send()
    for row in (1, 0):
        for flush in flushes(row):
            flush.wait()


def solution(mesh):
    stages = mesh.shape['stage']

    def device_step(tokens, targets, w_in, w_out, norm_gains):
        micro_count, tokens_mb, d_model = tokens.shape
        d_ff = w_in.shape[2]
        total = micro_count * tokens_mb
        count = total // CHUNK
        tokens = tokens.reshape(count, CHUNK, d_model)
        targets = targets.reshape(count, CHUNK, d_model)
        gains = norm_gains.reshape(2, 1, d_model)
        any_spec = pl.BlockSpec(memory_space=pl.ANY)
        vmem_spec = pl.BlockSpec(memory_space=pltpu.VMEM)
        dma = pltpu.SemaphoreType.DMA
        flops = 7 * 2 * 2 * total * d_model * d_ff
        grad_shape = jax.ShapeDtypeStruct((2, d_model, d_ff), F32)

        _, grad_in, grad_out_t, grad_gain, sse = pl.pallas_call(
            functools.partial(train_kernel, stages, 2.0 / total, LAGS),
            out_shape=(jax.ShapeDtypeStruct((4, count, CHUNK, d_model), BF16), grad_shape, grad_shape,
                       jax.ShapeDtypeStruct((2, 8, d_model), F32), jax.ShapeDtypeStruct((8, d_model), F32)),
            in_specs=[any_spec] * 4 + [vmem_spec],
            out_specs=(any_spec, any_spec, any_spec, vmem_spec, vmem_spec),
            scratch_shapes=[
                pltpu.VMEM((2, d_model, d_ff), BF16),
                pltpu.VMEM((2, F_BLK, d_model), BF16), pltpu.VMEM((3, F_BLK, d_model), BF16),
                pltpu.VMEM((2, d_model, d_ff), F32), pltpu.VMEM((2, d_model, d_ff), F32),
                pltpu.VMEM((2, CHUNK, d_model), BF16), pltpu.VMEM((2, CHUNK, d_model), BF16),
                pltpu.VMEM((2, CHUNK, d_model), BF16),
                pltpu.VMEM((CHUNK, d_model), BF16),
                pltpu.VMEM((d_model, CHUNK), BF16), pltpu.VMEM((d_model, CHUNK), BF16),
                pltpu.VMEM((CHUNK, d_model), F32),
                pltpu.VMEM((2, CHUNK, F_BLK), BF16), pltpu.VMEM((CHUNK, d_ff), BF16),
                dma((3,)), dma((3,)), dma((2,)), dma((2,)), dma((2, 2)), dma((4,)), dma((4, count)),
            ],
            compiler_params=pltpu.CompilerParams(collective_id=0, has_side_effects=True,
                                                 vmem_limit_bytes=VMEM_LIMIT),
            cost_estimate=pl.CostEstimate(flops=flops, bytes_accessed=10 ** 8, transcendentals=0),
        )(tokens, targets, w_in, w_out, gains)

        loss_value = lax.psum(jnp.sum(sse), 'stage') / (total * d_model)
        return grad_in, jnp.swapaxes(grad_out_t, 1, 2), jnp.sum(grad_gain, axis=1), loss_value.reshape(1)

    block_spec = P(('dp', 'stage'))
    return jax.shard_map(device_step, mesh=mesh,
                         in_specs=(P('dp'), P('dp'), P('stage'), P('stage'), P('stage')),
                         out_specs=(block_spec, block_spec, block_spec, P('dp')),
                         check_vma=False)
```
